256 devices in a mesh: rep: 4 (over z_hi), exp: 8 (over x, core), shard: 8 (over z_lo, y).
Axes of the slice: x: 4, y: 4, z: 8 (z_hi: 4, z_lo: 2; z = z_hi * 2 + z_lo), core: 2. Of those that a mesh axis runs over, the one named last changes fastest.
Arguments:
- tokens: bfloat16 [28672, 2048], P(('rep', 'exp', 'shard')), may hold values from -1.5 to 1.5
- routes: int32 [28672, 2], P(('rep', 'exp', 'shard')), may hold values from 0 to 7, all different within a row; in each aligned block of 112 rows (0 to 111, 112 to 223, ...) at most 31 rows name the same one
- gate_weight: bfloat16 [8, 2048, 7168], P('exp', None, 'shard'), may hold values from -0.125 to 0.125
- gate_cotangent: bfloat16 [8, 7936, 7168], P('exp', 'rep', 'shard'), may hold values from -0.75 to 0.75
Outputs:
- token_grad: bfloat16 [28672, 2048], P(('rep', 'exp', 'shard'))
- weight_grad: bfloat16 [8, 2048, 7168], P('exp', None, 'shard')
The draws below stay inside these ranges and needn't reach their ends.
Inputs may be any that keep to these rules, and one draw needn't show every extreme that they name: `routes`: the two entries of a row differ. The rows of one device name one expert at most 31 times, and some device names some expert exactly 31 times.
All inputs are finite; a program needn't handle non-finite values.
Results may differ from the reference program's by a relative error of at most 0.015.
Values may be sent and summed in bfloat16 or wider, within the bound.
A program may use at most 128 MiB of HBM per device.

```python
import math
import jax
import jax.numpy as jnp
import numpy as np
from jax import lax

DW = 2048
FFW = 7168
TOK_DEV = 112
EXPERTS = 8
TOKENS = 28672
SLOT_CAP = 31
SLOTS = 7936
N_REP = 4
N_EXP = 8
N_SHARD = 8


def shard_levels(rng, extent, pieces, least, high):
    gain = 1.0
    for dim, parts in pieces:
        steps = jax.random.uniform(jax.random.fold_in(jax.random.fold_in(rng, 6), dim), (parts,), jnp.float32, least / len(pieces), high / len(pieces))
        gain = gain * jnp.repeat(jnp.exp(steps), extent[dim] // parts).reshape((-1,) + (1,) * (len(extent) - 1 - dim))
    return gain


def routed_block(stream_key, own, number, rows, amount, top, most, lean):
    sequence = jax.random.permutation(stream_key, amount)
    packed, common = load_shares(amount, rows * top, most, lean, True), load_shares(amount, rows * top, most, lean, False)
    places = jnp.arange(amount)

    def named(tallies, rotation):
        used = int((tallies > 0).sum())
        fixed = max(1, used // 4)
        moved = fixed + (places - fixed + rotation * (used - fixed)) % max(1, amount - fixed)
        return jnp.zeros((amount,), jnp.int32).at[sequence[jnp.where(places < fixed, places, moved)]].set(jnp.asarray(tallies, jnp.int32))

    tallies = jnp.where(number % 4 == 0, named(packed, number // 4), named(common, number - number // 4 - 1))
    mixed = jax.random.permutation(jax.random.fold_in(own, 3), amount)
    source_of, taker = mixed[0:amount // 2 * 2:2], mixed[1:amount // 2 * 2:2]
    margin = jnp.minimum(tallies[source_of] - 1, most - tallies[taker]) // 2
    margin = jnp.where((source_of == sequence[0]) | (taker == sequence[0]) | (tallies[taker] == 0), 0, jnp.maximum(margin, 0))
    moved = jax.random.randint(jax.random.fold_in(own, 4), (amount // 2,), 0, 1 << 20) % (margin + 1)
    tallies = tallies.at[source_of].add(-moved).at[taker].add(moved)
    items = jnp.searchsorted(jnp.cumsum(tallies), jnp.arange(rows * top), side="right").astype(jnp.int32)
    listing = items.reshape(top, rows).T
    listing = listing[jax.random.permutation(jax.random.fold_in(own, 1), rows)]
    rotation = jax.random.randint(jax.random.fold_in(own, 2), (rows, 1), 0, top)
    return jnp.take_along_axis(listing, (jnp.arange(top)[None, :] + rotation) % top, axis=1)


def load_shares(number_of, total, limit, slope, full):
    portions = [(1 << 20) // math.isqrt(grade ** slope) + 1 for grade in range(1, number_of + 1)]
    largest = limit if full else min(limit, max(-(-total // number_of), total * portions[0] // sum(portions)))
    least = 1 if total - largest >= number_of - 1 else 0
    holding, surplus = [largest] + [least] * (number_of - 1), total - largest - least * (number_of - 1)
    while surplus > 0:
        free = [i for i in range(1, number_of) if holding[i] < largest] or [i for i in range(1, number_of) if holding[i] < limit]
        mass, left = sum([portions[i] for i in free]), surplus
        for i in free:
            more = min(limit - holding[i], max(1, left * portions[i] // mass), surplus)
            holding[i] = holding[i] + more
            surplus = surplus - more
    return np.array(holding)


def scatter_about(key, dims, spread, limit, split=(), kind=jnp.bfloat16):
    values = spread * jax.random.normal(key, dims, jnp.float32)
    if split:
        values = values * shard_levels(key, dims, split, -0.22, 0.18)
    return jnp.clip(values, -limit, limit).astype(kind)


def setup_inputs(seed: int = 0) -> dict:
    key_list = jax.random.split(jax.random.key(seed), 5)
    tokens = scatter_about(key_list[0], (TOKENS, DW), 0.25, 1.5, ((0, 256),))
    routes_keys = jax.random.split(jax.random.fold_in(key_list[1], 1), TOKENS // TOK_DEV)
    routes_turns = jax.random.permutation(jax.random.fold_in(key_list[1], 3), TOKENS // TOK_DEV)
    routes = jax.vmap(lambda own, number: routed_block(jax.random.fold_in(key_list[1], 2), own, number, TOK_DEV, EXPERTS, 2, SLOT_CAP, 2))(routes_keys, routes_turns).reshape((TOKENS, 2))
    gate_weight = scatter_about(key_list[2], (EXPERTS, DW, FFW), DW ** -0.5, 0.125, ((0, 8), (2, 8)))
    gate_cotangent = scatter_about(key_list[3], (EXPERTS, SLOTS, FFW), 0.125, 0.75, ((0, 8), (1, 4), (2, 8)))
    return {"tokens": tokens, "routes": routes, "gate_weight": gate_weight, "gate_cotangent": gate_cotangent}


def slot_matrix(route_rows, experts, slot_cap):
    expert_ids = jnp.arange(experts, dtype=jnp.int32)
    onehot = (route_rows[:, :, None] == expert_ids[None, None, :]).astype(jnp.int32)
    flattened = onehot.reshape(-1, experts)
    before = jnp.cumsum(flattened, axis=0) - flattened
    position = jnp.sum(before * flattened, axis=1)
    target = jnp.sum(flattened * expert_ids[None, :], axis=1) * slot_cap + position
    slot_ids = jnp.arange(experts * slot_cap, dtype=jnp.int32)
    matches = (target[None, :] == slot_ids[:, None]).astype(jnp.int32)
    return matches.reshape(experts * slot_cap, -1, 2).sum(axis=2)


def reference(tokens, routes, gate_weight, gate_cotangent):
    devices = N_REP * N_EXP * N_SHARD
    token_blocks = tokens.reshape(devices, TOK_DEV, DW).astype(jnp.float32)
    route_blocks = routes.reshape(devices, TOK_DEV, 2)

    def placing_of(route_rows):
        return slot_matrix(route_rows, EXPERTS, SLOT_CAP)

    placing = jax.vmap(placing_of)(route_blocks).astype(jnp.float32)
    outgoing = jnp.einsum("dst,dtw->dsw", placing, token_blocks).astype(jnp.bfloat16)
    grouped = outgoing.reshape(N_REP, N_EXP, N_SHARD, EXPERTS, SLOT_CAP, DW)
    grouped = grouped.transpose(3, 0, 1, 2, 4, 5).reshape(EXPERTS, SLOTS, DW)
    hidden_part = FFW // N_SHARD

    def per_expert(operands):
        gathered, cotangent, weights = operands
        weight_grad = jnp.dot(gathered.T, cotangent, preferred_element_type=jnp.float32).astype(jnp.bfloat16)
        summed = jnp.zeros((SLOTS, DW), jnp.float32)
        for shard_index in range(N_SHARD):
            lower = shard_index * hidden_part
            partial_value = jnp.dot(cotangent[:, lower:lower + hidden_part], weights[:, lower:lower + hidden_part].T,
                              preferred_element_type=jnp.float32).astype(jnp.bfloat16)
            partial_value = lax.optimization_barrier(partial_value)
            summed = summed + partial_value.astype(jnp.float32)
        return weight_grad, summed.astype(jnp.bfloat16)

    weight_grad, slot_grad = lax.map(per_expert, (grouped, gate_cotangent, gate_weight))
    returned = slot_grad.reshape(EXPERTS, N_REP, N_EXP, N_SHARD, SLOT_CAP, DW)
    returned = returned.transpose(1, 2, 3, 0, 4, 5).reshape(devices, EXPERTS * SLOT_CAP, DW)
    token_grad = jnp.einsum("dst,dsw->dtw", placing, returned.astype(jnp.float32)).astype(jnp.bfloat16)
    return token_grad.reshape(TOKENS, DW), weight_grad
```

```python
import functools

import jax
import jax.numpy as jnp
from jax import lax
from jax.experimental import pallas as pl
from jax.experimental.pallas import tpu as pltpu
from jax.sharding import PartitionSpec as P

MESH = pl.DeviceIdType.MESH
BF = jnp.bfloat16
F32 = jnp.float32
CHUNKS = 8
BLOCK = 32


def contract(a, b, da, db):
    return lax.dot_general(a, b, (((da,), (db,)), ((), ())), preferred_element_type=F32)


def kernel(
    sizes, tok, routes, w_hbm, c_hbm, tg_out, wg_out,
    cn, cp, wv, plt, tp, snd, g, prod, rr, u, x2, zs, zo, zr, acc, sb, rb,
    load_sem, pl_sem, t_sem, t_rsem, s_a, r_a, s_b, r_b, s_f, r_f, s_r, r_r, s_m, r_m, s_n, r_n, s_d, r_d, s_g, r_g,
):
    reps, experts, ys, slot_cap, width = sizes
    rep, me, shard = lax.axis_index("rep"), lax.axis_index("exp"), lax.axis_index("shard")
    zl, y = shard // ys, lax.rem(shard, ys)
    y_at = lambda k: lax.rem(y + k + 4 * ys, ys)
    r_at = lambda k: lax.rem(rep + k + 4 * reps, reps)
    y_to = ({"shard": zl * ys + y_at(1)}, {"shard": zl * ys + y_at(-1)})
    r_to = ({"rep": r_at(1)}, {"rep": r_at(-1)})
    z_to = {"shard": (1 - zl) * ys + y}
    exp_to = [{"exp": lax.rem(me + d, experts)} for d in range(1, experts)]
    others = experts - 1
    y_block = lambda k: (y_at(-1 - k), y_at(1 + k))
    r_block = lambda k: (r_at(-1 - k), r_at(1 + k))
    planes = (zl, 1 - zl)

    def rc(src, dst, ssem, rsem, dev):
        return pltpu.make_async_remote_copy(
            src_ref=src, dst_ref=dst, send_sem=ssem, recv_sem=rsem, device_id=dev, device_id_type=MESH
        )

    load_c = pltpu.make_async_copy(c_hbm, cn, load_sem.at[0])
    load_w = pltpu.make_async_copy(w_hbm, wv, load_sem.at[1])
    load_c.start()
    load_w.start()

    barrier = pltpu.get_barrier_semaphore()
    peers = [*y_to, *r_to, z_to, *exp_to]
    for dev in peers:
        pl.semaphore_signal(barrier, inc=1, device_id=dev, device_id_type=MESH)

    rows = tok.shape[0]
    slots = experts * BLOCK
    lane = lax.broadcasted_iota(jnp.int32, (rows, 128), 1)
    named = ((routes[:, 0:1] == lane) | (routes[:, 1:2] == lane)).astype(F32).astype(BF)
    before = (
        lax.broadcasted_iota(jnp.int32, (rows, rows), 1) < lax.broadcasted_iota(jnp.int32, (rows, rows), 0)
    ).astype(F32).astype(BF)
    position = contract(before, named, 1, 0).astype(BF)
    spread = (
        lax.broadcasted_iota(jnp.int32, (128, slots), 0) == lax.broadcasted_iota(jnp.int32, (128, slots), 1) // BLOCK
    ).astype(F32).astype(BF)
    slot_of = lax.rem(lax.broadcasted_iota(jnp.int32, (rows, slots), 1), BLOCK).astype(F32)
    hit = contract(named, spread, 1, 0)
    where = contract(position, spread, 1, 0)
    plt[0] = jnp.where(where == slot_of, hit, 0.0).astype(BF)

    pl.semaphore_wait(barrier, len(peers))

    send_pl = rc(plt.at[0], plt.at[1], pl_sem.at[0], pl_sem.at[1], z_to)
    send_pl.start()
    cols = lambda c: pl.ds(pl.multiple_of(c * width, 128), width)

    def send_tokens(c):
        return rc(tok.at[:, cols(c)], tp.at[:, cols(c)], t_sem.at[c], t_rsem.at[c], z_to)

    @pl.loop(0, CHUNKS)
    def _(c):
        send_tokens(c).start()

    load_c.wait()
    load_w.wait()

    row = lax.broadcasted_iota(jnp.int32, (2 * ys * BLOCK, 2 * ys * slot_cap), 0)
    col = lax.broadcasted_iota(jnp.int32, (2 * ys * BLOCK, 2 * ys * slot_cap), 1)
    inner = lax.rem(row, BLOCK)
    spaced = jnp.where((col == (row // BLOCK) * slot_cap + inner) & (inner < slot_cap), 1.0, 0.0).astype(BF)

    @pl.loop(0, experts)
    def _(e):
        moved = contract(spaced, cn[e], 1, 0).astype(BF)
        for z in range(2):
            for yy in range(ys):
                at = (z * ys + yy) * BLOCK
                cp[yy * 2 + z, e] = moved[at : at + BLOCK]

    slab = slots

    def a_copies(c, p):
        at = y * 2 + planes[p]
        return [
            rc(snd.at[c, p, dev["exp"]], g.at[c, at, me], s_a.at[c % 2, p], r_a.at[c, p], dev) for dev in exp_to
        ]

    def a_all(c, p):
        at = y * 2 + planes[p]
        return rc(g.at[c, at, pl.ds(0, others)], g.at[c, at, pl.ds(0, others)], s_a.at[c % 2, p], r_a.at[c, p], exp_to[0])

    def stage_a(c):
        for p in range(2):
            if p == 1:
                send_tokens(c).wait_recv()

                @pl.when(c == 0)
                def _():
                    send_pl.wait_recv()

            source = (tok, tp)[p][:, cols(c)]
            made = contract(plt[p], source, 0, 0).astype(BF).reshape(experts, BLOCK, width)
            snd[c, p] = made
            g[c, y * 2 + planes[p], me] = snd[c, p, me]
            for copy in a_copies(c, p):
                copy.start()

    def b_copies(c):
        return [
            rc(g.at[c, y * 2 + p], g.at[c, y * 2 + p], s_b.at[c % 2, d, p], r_b.at[c, d, p], y_to[d])
            for p in range(2)
            for d in range(2)
        ]

    def b_arrived(c, d, p):
        at = (y_at(-1), y_at(1))[d] * 2 + p
        return rc(g.at[c, at], g.at[c, at], s_b.at[c % 2, d, p], r_b.at[c, d, p], y_to[d])

    def f_copies(c):
        out = []
        for d in range(2):
            at = (y_at(-1), y_at(1))[d] * 2 + d
            out.append(rc(g.at[c, at], g.at[c, at], s_f.at[c % 2, d], r_f.at[c, d], y_to[d]))
        return out

    def stage_b(c):
        for p in range(2):
            a_all(c, p).wait_recv()
        for copy in b_copies(c):
            copy.start()

    def stage_f(c):
        copies = f_copies(c)
        for d in range(2):
            b_arrived(c, d, d).wait_recv()
            copies[d].start()

    def stage_w(c):
        b_arrived(c, 0, 1).wait_recv()
        b_arrived(c, 1, 0).wait_recv()
        for copy in f_copies(c):
            copy.wait_recv()
        grad = contract(g[c].reshape(2 * ys * slab, width), cp[...].reshape(2 * ys * slab, -1), 0, 0)
        acc[c % 2] = grad.reshape(2 * reps, width // (2 * reps), -1)
        for d in range(2):
            sb[c % 2, d] = acc[c % 2, r_block(0)[d] * 2 + d].astype(BF)
        for copy in d_copies(c, 0):
            copy.start()

    def d_copies(c, k):
        return [
            rc(sb.at[c % 2, d] if k == 0 else rb.at[c, k - 1, d], rb.at[c, k, d], s_d.at[c % 2, k, d], r_d.at[c, k, d], r_to[d])
            for d in range(2)
        ]

    def stage_d(c, k):
        came, send = d_copies(c, k - 1), d_copies(c, k)
        for d in range(2):
            came[d].wait_recv()
            rb[c, k - 1, d] = (rb[c, k - 1, d].astype(F32) + acc[c % 2, r_block(k)[d] * 2 + d]).astype(BF)
            send[d].start()

    def g_copies(c, k):
        out = []
        for d in range(2):
            at = (r_at(-k), r_at(k))[d] * 2 + d
            out.append(rc(wg_out.at[c, at], wg_out.at[c, at], s_g.at[c % 2, k, d], r_g.at[c, k, d], r_to[d]))
        return out

    def stage_e(c):
        came, send = d_copies(c, 2), g_copies(c, 0)
        for d in range(2):
            came[d].wait_recv()
            wg_out[c, rep * 2 + d] = (rb[c, 2, d].astype(F32) + acc[c % 2, rep * 2 + d]).astype(BF)
            send[d].start()

    def stage_g(c, k):
        came, send = g_copies(c, k - 1), g_copies(c, k)
        for d in range(2):
            came[d].wait_recv()
            send[d].start()

    def stage_end(c):
        for copy in g_copies(c, 2):
            copy.wait_recv()

    def r_copies(c, k):
        out = []
        for d in range(2):
            src = prod.at[c % 2, y_block(0)[d] * 2 + d] if k == 0 else rr.at[c, k - 1, d]
            out.append(rc(src, rr.at[c, k, d], s_r.at[c % 2, k, d], r_r.at[c, k, d], y_to[d]))
        return out

    def stage_p(c):
        weights = wv[cols(c), :]

        @pl.loop(0, 2 * ys)
        def _(s):
            prod[c % 2, s] = contract(cp[s].reshape(slab, -1), weights, 1, 1).astype(BF)

        for copy in r_copies(c, 0):
            copy.start()

    def stage_r(c, k):
        came, send = r_copies(c, k - 1), r_copies(c, k)
        for d in range(2):
            came[d].wait_recv()
            rr[c, k - 1, d] = (rr[c, k - 1, d].astype(F32) + prod[c % 2, y_block(k)[d] * 2 + d].astype(F32)).astype(BF)
            send[d].start()

    def m_copies(c, d):
        return [rc(u.at[c, d, dev["exp"]], x2.at[c, d, me], s_m.at[c % 2, d], r_m.at[c, d], dev) for dev in exp_to]

    def m_all(c, d):
        return rc(x2.at[c, d, pl.ds(0, others)], x2.at[c, d, pl.ds(0, others)], s_m.at[c % 2, d], r_m.at[c, d], exp_to[0])

    def stage_m(c):
        came = r_copies(c, 2)
        for d in range(2):
            came[d].wait_recv()
            total = rr[c, 2, d].astype(F32) + prod[c % 2, y * 2 + d].astype(F32)
            u[c, d] = total.astype(BF).reshape(experts, BLOCK, width)
            x2[c, d, me] = u[c, d, me]
            for copy in m_copies(c, d):
                copy.start()

    def n_copy(c):
        return rc(zs.at[c], zr.at[c], s_n.at[c % 2], r_n.at[c], z_to)

    def stage_n(c):
        for d in range(2):
            m_all(c, d).wait_recv()
        theirs = contract(plt[1], x2[c, planes[1]].reshape(slots, width), 1, 0)
        zs[c] = theirs.astype(BF)
        n_copy(c).start()
        zo[c] = contract(plt[0], x2[c, planes[0]].reshape(slots, width), 1, 0)

    def stage_o(c):
        n_copy(c).wait_recv()
        tg_out[:, cols(c)] = (zo[c] + zr[c].astype(F32)).astype(BF)

    def at(t, offset, stage):
        c = t - offset

        @pl.when((c >= 0) & (c < CHUNKS))
        def _():
            stage(c)

    def wait_sends(make):
        def stage(c):
            for copy in make(c):
                copy.wait_send()

        return stage

    first = 1

    @pl.loop(0, CHUNKS + first + 4)
    def _(t):
        at(t, first, stage_p)
        at(t, 1, stage_b)
        at(t, 0, stage_a)
        at(t, 2, stage_w)
        at(t, first + 1, stage_m)
        at(t, 3, stage_e)
        at(t, first + 2, stage_n)
        at(t, first + 3, stage_o)

        at(t, first, functools.partial(stage_r, k=1))
        at(t, 1, stage_f)
        at(t, 2, functools.partial(stage_d, k=1))
        at(t, 3, functools.partial(stage_g, k=1))
        at(t, 1, wait_sends(lambda c: [a_all(c, 0), a_all(c, 1)]))
        at(t, 2, wait_sends(lambda c: b_copies(c) + f_copies(c)))
        at(t, 3, wait_sends(lambda c: d_copies(c, 0) + d_copies(c, 1) + d_copies(c, 2)))
        at(t, 4, wait_sends(lambda c: g_copies(c, 0) + g_copies(c, 1) + g_copies(c, 2)))
        at(t, first + 1, wait_sends(lambda c: r_copies(c, 0) + r_copies(c, 1) + r_copies(c, 2)))
        at(t, first + 2, wait_sends(lambda c: [m_all(c, 0), m_all(c, 1)]))
        at(t, first + 3, wait_sends(lambda c: [n_copy(c), send_tokens(c)]))

        at(t, first, functools.partial(stage_r, k=2))
        at(t, 2, functools.partial(stage_d, k=2))
        at(t, 3, functools.partial(stage_g, k=2))
        at(t, 4, stage_end)

    send_pl.wait_send()


def solution(mesh):
    reps, experts, shards = (mesh.shape[a] for a in ("rep", "exp", "shard"))
    ys = shards // 2

    def body(tokens, routes, gate_weight, gate_cotangent):
        rows, features = tokens.shape
        hidden = gate_weight.shape[2]
        slot_cap = gate_cotangent.shape[1] // (experts * shards)
        width = features // CHUNKS
        n = CHUNKS
        slots = experts * BLOCK
        cotangent = gate_cotangent.reshape(experts, shards * slot_cap, hidden)
        vmem = lambda *shape: pltpu.VMEM(shape, BF)
        wide = lambda *shape: pltpu.VMEM(shape, F32)
        dma = lambda *shape: pltpu.SemaphoreType.DMA(shape)
        whole = pl.BlockSpec(memory_space=pltpu.VMEM)
        far = pl.BlockSpec(memory_space=pl.ANY)
        piece = width // (2 * reps)
        scratch = [
            vmem(experts, shards * slot_cap, hidden),
            vmem(shards, experts, BLOCK, hidden),
            vmem(features, hidden),
            vmem(2, rows, slots),
            vmem(rows, features),
            vmem(n, 2, experts, BLOCK, width),
            vmem(n, shards, experts, BLOCK, width),
            vmem(2, shards, slots, width),
            vmem(n, 3, 2, slots, width),
            vmem(n, 2, experts, BLOCK, width),
            vmem(n, 2, experts, BLOCK, width),
            vmem(n, rows, width),
            wide(n, rows, width),
            vmem(n, rows, width),
            wide(2, 2 * reps, piece, hidden),
            vmem(2, 2, piece, hidden),
            vmem(n, 3, 2, piece, hidden),
            dma(2), dma(2), dma(n), dma(n),
            dma(2, 2), dma(n, 2),
            dma(2, 2, 2), dma(n, 2, 2),
            dma(2, 2), dma(n, 2),
            dma(2, 3, 2), dma(n, 3, 2),
            dma(2, 2), dma(n, 2),
            dma(2), dma(n),
            dma(2, 3, 2), dma(n, 3, 2),
            dma(2, 3, 2), dma(n, 3, 2),
        ]
        token_grad, weight_grad = pl.pallas_call(
            functools.partial(kernel, (reps, experts, ys, slot_cap, width)),
            out_shape=(
                jax.ShapeDtypeStruct((rows, features), BF),
                jax.ShapeDtypeStruct((n, 2 * reps, piece, hidden), BF),
            ),
            in_specs=[whole, whole, far, far],
            out_specs=(whole, whole),
            scratch_shapes=scratch,
            compiler_params=pltpu.CompilerParams(
                collective_id=0, has_side_effects=True, vmem_limit_bytes=67_000_000
            ),
            name="moe_gate_backward",
        )(tokens, routes, gate_weight[0], cotangent)
        return token_grad, weight_grad.reshape(1, features, hidden)

    spec = P(("rep", "exp", "shard"), None)
    return jax.shard_map(
        body,
        mesh=mesh,
        in_specs=(spec, spec, P("exp", None, "shard"), P("exp", "rep", "shard")),
        out_specs=(spec, P("exp", None, "shard")),
        check_vma=False,
    )
```

```python
import functools

import jax
import jax.numpy as jnp
from jax import lax
from jax.experimental import pallas as pl
from jax.experimental.pallas import tpu as pltpu
from jax.sharding import PartitionSpec as P

MESH = pl.DeviceIdType.MESH
BF = jnp.bfloat16
F32 = jnp.float32
CHUNKS = 16
EARLY = 3
KEEP = 8
VMEM = 50_000_000
BLOCK = 32


def contract(a, b, da, db):
    return lax.dot_general(a, b, (((da,), (db,)), ((), ())), preferred_element_type=F32)


def kernel(
    sizes, tok_hbm, routes_hbm, c_hbm, w_hbm, tg_out, wg_out,
    tok, routes, cn, cp, wv, pls, tp, snd, g, prod, rr, rr1, u, x2, zs, zo, zr, acc, sb, rb, rc1,
    load_sem, pl_sem, t_sem, t_rsem, s_z, r_z, s_a, r_a, s_b, r_b, s_f, r_f, s_r, r_r, s_m, r_m, s_n, r_n, s_d, r_d, s_g, r_g,
):
    reps, experts, ys, slot_cap, width = sizes
    rep, me, shard = lax.axis_index("rep"), lax.axis_index("exp"), lax.axis_index("shard")
    zl, y = shard // ys, lax.rem(shard, ys)
    y_at = lambda k: lax.rem(y + k + 4 * ys, ys)
    swap = lambda i: (i + 1 - 2 * lax.rem(i, 2), 3 - i)
    bits = lambda i: (lax.rem((i + 1) // 2, 2), i // 2)
    y_pair, r_pair = swap(y), swap(rep)
    y_far = lax.rem(y + 2, ys)
    r_bit = bits(rep)
    y_to = ({"shard": zl * ys + y_at(1)}, {"shard": zl * ys + y_at(-1)})
    y_by = tuple({"shard": zl * ys + i} for i in y_pair)
    r_by = tuple({"rep": i} for i in r_pair)
    z_to = {"shard": (1 - zl) * ys + y}
    exp_to = [{"exp": lax.rem(me + d, experts)} for d in range(1, experts)]
    others = experts - 1
    planes = (zl, 1 - zl)

    def rc(src, dst, ssem, rsem, dev):
        return pltpu.make_async_remote_copy(
            src_ref=src, dst_ref=dst, send_sem=ssem, recv_sem=rsem, device_id=dev, device_id_type=MESH
        )

    loads = [
        pltpu.make_async_copy(src, dst, load_sem.at[i])
        for i, (src, dst) in enumerate(((routes_hbm, routes), (tok_hbm, tok), (c_hbm, cn), (w_hbm, wv)))
    ]
    for load in loads:
        load.start()

    barrier = pltpu.get_barrier_semaphore()
    cross_to = [{**dev, **z_to} for dev in exp_to]
    peers = [*y_to, *r_by, z_to, *exp_to, *cross_to]
    for dev in peers:
        pl.semaphore_signal(barrier, inc=1, device_id=dev, device_id_type=MESH)

    loads[0].wait()
    rows = tok.shape[0]
    slots = experts * BLOCK
    name = lax.broadcasted_iota(jnp.int32, (experts, rows), 0)
    named = ((routes[0:1, :] == name) | (routes[1:2, :] == name)).astype(F32).astype(BF)
    before = (
        lax.broadcasted_iota(jnp.int32, (rows, rows), 0) < lax.broadcasted_iota(jnp.int32, (rows, rows), 1)
    ).astype(F32).astype(BF)
    position = contract(named, before, 1, 0).astype(BF)
    spread = (
        lax.broadcasted_iota(jnp.int32, (slots, experts), 0) // BLOCK
        == lax.broadcasted_iota(jnp.int32, (slots, experts), 1)
    ).astype(F32).astype(BF)
    slot_of = lax.rem(lax.broadcasted_iota(jnp.int32, (slots, rows), 0), BLOCK).astype(F32)
    hit = contract(spread, named, 1, 0)
    where = contract(spread, position, 1, 0)
    pls[0] = jnp.where(where == slot_of, hit, 0.0).astype(BF)

    pl.semaphore_wait(barrier, len(peers))

    send_pl = rc(pls.at[0], pls.at[1], pl_sem.at[0], pl_sem.at[1], z_to)
    loads[1].wait()
    cols = lambda c: pl.ds(pl.multiple_of(c * width, 128), width)

    def send_tokens(c):
        return rc(tok.at[:, cols(c)], tp.at[:, cols(c)], t_sem.at[c], t_rsem.at[c], z_to)

    slab = slots

    def a_copies(c, p):
        at = y * 2 + planes[p]
        return [
            rc(snd.at[c % 4, p, dev["exp"]], g.at[c, at, me], s_a.at[c % 4, p], r_a.at[c, p], dev) for dev in exp_to
        ]

    def a_all(c, p):
        at = y * 2 + planes[p]
        return rc(g.at[c, at, pl.ds(0, others)], g.at[c, at, pl.ds(0, others)], s_a.at[c % 4, p], r_a.at[c, p], exp_to[0])

    def pair_copy(c, slot):
        return rc(snd.at[slot, 0, me], g.at[c, y * 2 + zl, me], s_z.at[c], r_z.at[c], z_to)

    def pair_came(c):
        block = g.at[c, y * 2 + 1 - zl, me]
        return rc(block, block, s_z.at[c], r_z.at[c], z_to)

    def early_a(c):
        snd[c, 0] = contract(pls[0], tok[:, cols(c)], 1, 0).astype(BF).reshape(experts, BLOCK, width)
        g[c, y * 2 + zl, me] = snd[c, 0, me]
        for copy in a_copies(c, 0):
            copy.start()
        for dev in cross_to:
            rc(snd.at[c, 0, dev["exp"]], g.at[c, y * 2 + zl, me], s_a.at[c, 1], r_a.at[c, 1], dev).start()
        pair_copy(c, c).start()

    def stage_a(c, p):
        if p == 1:
            send_tokens(c).wait_recv()

            @pl.when(c == EARLY)
            def _():
                send_pl.wait_recv()

        source = (tok, tp)[p][:, cols(c)]
        made = contract(pls[p], source, 1, 0).astype(BF).reshape(experts, BLOCK, width)
        snd[c % 4, p] = made
        g[c, y * 2 + planes[p], me] = snd[c % 4, p, me]
        for copy in a_copies(c, p):
            copy.start()

    def early_only(c, do):
        if isinstance(c, int):
            do()
        else:
            pl.when(c < EARLY)(do)

    def b_copies(c):
        return [
            rc(g.at[c, y * 2 + p], g.at[c, y * 2 + p], s_b.at[c % 2, d, p], r_b.at[c, d, p], y_to[d])
            for d, p in ((0, 0), (1, 1), (0, 1), (1, 0))
        ]

    def b_arrived(c, d, p):
        at = (y_at(-1), y_at(1))[d] * 2 + p
        return rc(g.at[c, at], g.at[c, at], s_b.at[c % 2, d, p], r_b.at[c, d, p], y_to[d])

    def f_copies(c):
        out = []
        for d in range(2):
            at = (y_at(-1), y_at(1))[d] * 2 + d
            out.append(rc(g.at[c, at], g.at[c, at], s_f.at[c % 2, d], r_f.at[c, d], y_to[d]))
        return out

    def stage_b(c):
        for p in range(2):
            a_all(c, p).wait_recv()
        early_only(c, lambda: pair_came(c).wait_recv())
        for copy in b_copies(c):
            copy.start()

    def stage_f(c):
        copies = f_copies(c)
        for d in range(2):
            b_arrived(c, d, d).wait_recv()
            copies[d].start()

    def stage_w(c):
        b_arrived(c, 0, 1).wait_recv()
        b_arrived(c, 1, 0).wait_recv()
        for copy in f_copies(c):
            copy.wait_recv()
        grad = contract(g[c].reshape(2 * ys * slab, width), cp[...].reshape(2 * ys * slab, -1), 0, 0)
        acc[c % 4] = grad.reshape(2, 2, 2, width // 8, -1)
        for v in range(2):
            sb[c % 4, v] = acc[c % 4, v, 1 - r_bit[v]].astype(BF)
        for copy in d0_copies(c):
            copy.start()

    def d0_copies(c):
        return [rc(sb.at[c % 4, v], rb.at[c, v], s_d.at[c % 2, 0, v], r_d.at[c, 0, v], r_by[v]) for v in range(2)]

    def d1_copies(c):
        return [
            rc(rb.at[c, v, 1 - r_bit[1 - v]], rc1.at[c, v], s_d.at[c % 2, 1, v], r_d.at[c, 1, v], r_by[1 - v])
            for v in range(2)
        ]

    def stage_d(c):
        came, send = d0_copies(c), d1_copies(c)
        for v in range(2):
            came[v].wait_recv()
            q = 1 - r_bit[1 - v]
            rb[c, v, q] = (rb[c, v, q].astype(F32) + acc[c % 4, v, r_bit[v], q]).astype(BF)
            send[v].start()

    def g0_copies(c):
        out = []
        for v in range(2):
            piece = wg_out.at[c, v, r_bit[v], r_bit[1 - v]]
            out.append(rc(piece, piece, s_g.at[c % 2, 0, v], r_g.at[c, 0, v], r_by[1 - v]))
        return out

    def g1_copies(c):
        out = []
        for v in range(2):
            half = wg_out.at[c, v, r_bit[v]]
            out.append(rc(half, half, s_g.at[c % 2, 1, v], r_g.at[c, 1, v], r_by[v]))
        return out

    def stage_e(c):
        came, send = d1_copies(c), g0_copies(c)
        for v in range(2):
            came[v].wait_recv()
            h, q = r_bit[v], r_bit[1 - v]
            total = acc[c % 4, v, h, q] + rb[c, v, q].astype(F32) + rc1[c, v].astype(F32)
            wg_out[c, v, h, q] = total.astype(BF)
            send[v].start()

    def stage_g(c):
        came, send = g0_copies(c), g1_copies(c)
        for v in range(2):
            came[v].wait_recv()
            send[v].start()

    def stage_end(c):
        for copy in g1_copies(c):
            copy.wait_recv()

    def r0_copies(c):
        return [
            rc(prod.at[c % KEEP, (y_pair[v], y_far)[i] * 2 + v], rr.at[c, v, i], s_r.at[c % 2, i, v], r_r.at[c, i, v], y_by[v])
            for i in (1, 0)
            for v in range(2)
        ]

    def r1_copies(c):
        return [rc(rr.at[c, v, 1], rr1.at[c, v], s_r.at[c % 2, 2, v], r_r.at[c, 2, v], y_by[1 - v]) for v in range(2)]

    def stage_p(c):
        odd = lax.rem(c, 2)
        pair = c - odd
        weights = wv[pl.ds(pl.multiple_of(pair * width, 256), 2 * width), :]

        @pl.loop(0, ys)
        def _(i):
            s = odd * ys + i
            made = contract(cp[s].reshape(slab, -1), weights, 1, 1).astype(BF)
            for j in range(2):
                prod[lax.rem(pair + j, KEEP), s] = made[:, j * width : (j + 1) * width]

    def stage_r0(c):
        for copy in r0_copies(c):
            copy.start()

    def stage_r1(c):
        came, send = r0_copies(c), r1_copies(c)
        for v in range(2):
            came[v].wait_recv()
            mine = prod[c % KEEP, y_pair[1 - v] * 2 + v].astype(F32)
            rr[c, v, 1] = (rr[c, v, 1].astype(F32) + mine).astype(BF)
            send[v].start()

    def m_copies(c, d):
        return [rc(u.at[c % 4, d, dev["exp"]], x2.at[c, d, me], s_m.at[c % 2, d], r_m.at[c, d], dev) for dev in exp_to]

    def m_all(c, d):
        return rc(x2.at[c, d, pl.ds(0, others)], x2.at[c, d, pl.ds(0, others)], s_m.at[c % 2, d], r_m.at[c, d], exp_to[0])

    def stage_m(c):
        first_half, second = r0_copies(c), r1_copies(c)
        for d in range(2):
            first_half[2 + d].wait_recv()
            second[d].wait_recv()
            total = rr[c, d, 0].astype(F32) + prod[c % KEEP, y * 2 + d].astype(F32) + rr1[c, d].astype(F32)
            u[c % 4, d] = total.astype(BF).reshape(experts, BLOCK, width)
            x2[c, d, me] = u[c % 4, d, me]
            for copy in m_copies(c, d):
                copy.start()

    def n_copy(c):
        return rc(zs.at[c], zr.at[c], s_n.at[c % 2], r_n.at[c], z_to)

    def stage_n(c):
        for d in range(2):
            m_all(c, d).wait_recv()
        theirs = contract(pls[1], x2[c, planes[1]].reshape(slots, width), 0, 0)
        zs[c] = theirs.astype(BF)
        n_copy(c).start()
        zo[c] = contract(pls[0], x2[c, planes[0]].reshape(slots, width), 0, 0)

    def stage_o(c):
        n_copy(c).wait_recv()
        tg_out[:, cols(c)] = (zo[c] + zr[c].astype(F32)).astype(BF)

    def at(t, offset, stage):
        c = t - offset

        @pl.when((c >= 0) & (c < CHUNKS))
        def _():
            stage(c)

    def wait_sends(make):
        def stage(c):
            for copy in make(c):
                copy.wait_send()

        return stage

    def prepare():
        loads[2].wait()
        row = lax.broadcasted_iota(jnp.int32, (2 * ys * BLOCK, 2 * ys * slot_cap), 0)
        col = lax.broadcasted_iota(jnp.int32, (2 * ys * BLOCK, 2 * ys * slot_cap), 1)
        inner = lax.rem(row, BLOCK)
        spaced = jnp.where((col == (row // BLOCK) * slot_cap + inner) & (inner < slot_cap), 1.0, 0.0).astype(BF)

        @pl.loop(0, experts)
        def _(e):
            moved = contract(spaced, cn[e], 1, 0).astype(BF)
            for z in range(2):
                for yy in range(ys):
                    at = (z * ys + yy) * BLOCK
                    cp[yy * 2 + z, e] = moved[at : at + BLOCK]

    first = 3
    ticks = CHUNKS + max(first + 5, 7)

    early_a(0)
    send_pl.start()
    for c in range(1, EARLY):
        early_a(c)

    @pl.loop(EARLY, CHUNKS)
    def _(c):
        send_tokens(c).start()

    prepare()
    loads[3].wait()
    stage_b(0)
    a_all(0, 0).wait_send()
    a_all(0, 1).wait_send()
    pair_copy(0, 0).wait_send()

    @pl.loop(1, ticks)
    def _(t):
        at(t, 6, stage_end)
        at(t, first + 2, stage_m)
        at(t, 5, stage_g)
        at(t, first + 1, stage_r1)
        at(t, 4, stage_e)
        at(t, 1, stage_f)
        at(t, 3, stage_d)
        at(t, first, stage_r0)
        at(t, 0, stage_b)
        at(t, 2, stage_w)
        at(t, first + 3, stage_n)
        at(t, first + 4, stage_o)
        at(t, -2, functools.partial(stage_a, p=0))
        at(t, -2, functools.partial(stage_a, p=1))
        at(t, 0, wait_sends(lambda c: [a_all(c, 0), a_all(c, 1)]))
        at(t, 0, lambda c: early_only(c, lambda: pair_copy(c, c % 4).wait_send()))
        at(t, 1, wait_sends(lambda c: b_copies(c)))
        at(t, 2, wait_sends(lambda c: f_copies(c)))
        at(t, 3, wait_sends(lambda c: d0_copies(c)))
        at(t, 4, wait_sends(lambda c: d1_copies(c)))
        at(t, 5, wait_sends(lambda c: g0_copies(c)))
        at(t, 6, wait_sends(lambda c: g1_copies(c)))
        at(t, first + 1, wait_sends(lambda c: r0_copies(c)))
        at(t, first + 2, wait_sends(lambda c: r1_copies(c)))
        at(t, first + 3, wait_sends(lambda c: [m_all(c, 0), m_all(c, 1)]))
        at(t, first + 4, wait_sends(lambda c: [n_copy(c)]))
        at(t, first + 4, lambda c: pl.when(c >= EARLY)(lambda: send_tokens(c).wait_send()))
        at(t, first - 2, stage_p)

    send_pl.wait_send()


def solution(mesh):
    reps, experts, shards = (mesh.shape[a] for a in ("rep", "exp", "shard"))
    ys = shards // 2

    def body(tokens, routes, gate_weight, gate_cotangent):
        rows, features = tokens.shape
        hidden = gate_weight.shape[2]
        slot_cap = gate_cotangent.shape[1] // (experts * shards)
        width = features // CHUNKS
        n = CHUNKS
        slots = experts * BLOCK
        cotangent = gate_cotangent.reshape(experts, shards * slot_cap, hidden)
        vmem = lambda *shape: pltpu.VMEM(shape, BF)
        wide = lambda *shape: pltpu.VMEM(shape, F32)
        dma = lambda *shape: pltpu.SemaphoreType.DMA(shape)
        whole = pl.BlockSpec(memory_space=pltpu.VMEM)
        far = pl.BlockSpec(memory_space=pltpu.HBM)
        piece = width // 8
        scratch = [
            vmem(rows, features),
            pltpu.VMEM((2, rows), jnp.int32),
            vmem(experts, shards * slot_cap, hidden),
            vmem(shards, experts, BLOCK, hidden),
            vmem(features, hidden),
            vmem(2, slots, rows),
            vmem(rows, features),
            vmem(4, 2, experts, BLOCK, width),
            vmem(n, shards, experts, BLOCK, width),
            vmem(KEEP, shards, slots, width),
            vmem(n, 2, 2, slots, width),
            vmem(n, 2, slots, width),
            vmem(4, 2, experts, BLOCK, width),
            vmem(n, 2, experts, BLOCK, width),
            vmem(n, rows, width),
            wide(n, rows, width),
            vmem(n, rows, width),
            wide(4, 2, 2, 2, piece, hidden),
            vmem(4, 2, 2, piece, hidden),
            vmem(n, 2, 2, piece, hidden),
            vmem(n, 2, piece, hidden),
            dma(4), dma(2), dma(n), dma(n), dma(EARLY), dma(EARLY),
            dma(4, 2), dma(n, 2),
            dma(2, 2, 2), dma(n, 2, 2),
            dma(2, 2), dma(n, 2),
            dma(2, 3, 2), dma(n, 3, 2),
            dma(2, 2), dma(n, 2),
            dma(2), dma(n),
            dma(2, 2, 2), dma(n, 2, 2),
            dma(2, 2, 2), dma(n, 2, 2),
        ]
        token_grad, weight_grad = pl.pallas_call(
            functools.partial(kernel, (reps, experts, ys, slot_cap, width)),
            out_shape=(
                jax.ShapeDtypeStruct((rows, features), BF),
                jax.ShapeDtypeStruct((n, 2, 2, 2, piece, hidden), BF),
            ),
            in_specs=[far, far, far, far],
            out_specs=(whole, whole),
            scratch_shapes=scratch,
            compiler_params=pltpu.CompilerParams(
                collective_id=0, has_side_effects=True, vmem_limit_bytes=VMEM
            ),
            name="moe_gate_backward",
        )(*(pltpu.with_memory_space_constraint(a, pltpu.HBM) for a in (tokens, routes.T, cotangent, gate_weight[0])))
        return token_grad, weight_grad.reshape(1, features, hidden)

    spec = P(("rep", "exp", "shard"), None)
    return jax.shard_map(
        body,
        mesh=mesh,
        in_specs=(spec, spec, P("exp", None, "shard"), P("exp", "rep", "shard")),
        out_specs=(spec, P("exp", None, "shard")),
        check_vma=False,
    )
```

```python
import functools

import jax
import jax.numpy as jnp
from jax import lax
from jax.experimental import pallas as pl
from jax.experimental.pallas import tpu as pltpu
from jax.sharding import PartitionSpec as P

MESH = pl.DeviceIdType.MESH
BF = jnp.bfloat16
F32 = jnp.float32
CHUNKS = 16
EARLY = 3
KEEP = 8
VMEM = 50_000_000
BLOCK = 32


def contract(a, b, da, db):
    return lax.dot_general(a, b, (((da,), (db,)), ((), ())), preferred_element_type=F32)


def kernel(
    sizes, tok_hbm, routes_hbm, c_hbm, w_hbm, tg_out, wg_out,
    tok, routes, cn, cp, wv, pls, tp, snd, g, prod, rr, rr1, u, x2, zs, zo, zr, acc, sb, rb, rc1,
    load_sem, pl_sem, t_sem, t_rsem, s_z, r_z, s_a, r_a, s_b, r_b, s_f, r_f, s_r, r_r, s_m, r_m, s_n, r_n, s_d, r_d, s_g, r_g,
):
    reps, experts, ys, slot_cap, width = sizes
    rep, me, shard = lax.axis_index("rep"), lax.axis_index("exp"), lax.axis_index("shard")
    zl, y = shard // ys, lax.rem(shard, ys)
    y_at = lambda k: lax.rem(y + k + 4 * ys, ys)
    swap = lambda i: (i + 1 - 2 * lax.rem(i, 2), 3 - i)
    bits = lambda i: (lax.rem((i + 1) // 2, 2), i // 2)
    y_pair, r_pair = swap(y), swap(rep)
    y_far = lax.rem(y + 2, ys)
    r_bit = bits(rep)
    y_to = ({"shard": zl * ys + y_at(1)}, {"shard": zl * ys + y_at(-1)})
    y_by = tuple({"shard": zl * ys + i} for i in y_pair)
    r_by = tuple({"rep": i} for i in r_pair)
    z_to = {"shard": (1 - zl) * ys + y}
    exp_to = [{"exp": lax.rem(me + d, experts)} for d in range(1, experts)]
    others = experts - 1
    planes = (zl, 1 - zl)

    def rc(src, dst, ssem, rsem, dev):
        return pltpu.make_async_remote_copy(
            src_ref=src, dst_ref=dst, send_sem=ssem, recv_sem=rsem, device_id=dev, device_id_type=MESH
        )

    loads = [
        pltpu.make_async_copy(src, dst, load_sem.at[i])
        for i, (src, dst) in enumerate(((routes_hbm, routes), (tok_hbm, tok), (c_hbm, cn), (w_hbm, wv)))
    ]
    for load in loads:
        load.start()

    barrier = pltpu.get_barrier_semaphore()
    cross_to = [{**dev, **z_to} for dev in exp_to]
    peers = [*y_to, *r_by, z_to, *exp_to, *cross_to]
    for dev in peers:
        pl.semaphore_signal(barrier, inc=1, device_id=dev, device_id_type=MESH)

    loads[0].wait()
    rows = tok.shape[0]
    slots = experts * BLOCK
    name = lax.broadcasted_iota(jnp.int32, (experts, rows), 0)
    named = ((routes[0:1, :] == name) | (routes[1:2, :] == name)).astype(F32).astype(BF)
    before = (
        lax.broadcasted_iota(jnp.int32, (rows, rows), 0) < lax.broadcasted_iota(jnp.int32, (rows, rows), 1)
    ).astype(F32).astype(BF)
    position = contract(named, before, 1, 0).astype(BF)
    spread = (
        lax.broadcasted_iota(jnp.int32, (slots, experts), 0) // BLOCK
        == lax.broadcasted_iota(jnp.int32, (slots, experts), 1)
    ).astype(F32).astype(BF)
    slot_of = lax.rem(lax.broadcasted_iota(jnp.int32, (slots, rows), 0), BLOCK).astype(F32)
    hit = contract(spread, named, 1, 0)
    where = contract(spread, position, 1, 0)
    pls[0] = jnp.where(where == slot_of, hit, 0.0).astype(BF)

    pl.semaphore_wait(barrier, len(peers))

    send_pl = rc(pls.at[0], pls.at[1], pl_sem.at[0], pl_sem.at[1], z_to)
    loads[1].wait()
    cols = lambda c: pl.ds(pl.multiple_of(c * width, 128), width)

    def send_tokens(c):
        return rc(tok.at[:, cols(c)], tp.at[:, cols(c)], t_sem.at[c], t_rsem.at[c], z_to)

    slab = slots

    def a_copies(c, p):
        at = y * 2 + planes[p]
        return [
            rc(snd.at[c % 4, p, dev["exp"]], g.at[c, at, me], s_a.at[c % 4, p], r_a.at[c, p], dev) for dev in exp_to
        ]

    def a_all(c, p):
        at = y * 2 + planes[p]
        return rc(g.at[c, at, pl.ds(0, others)], g.at[c, at, pl.ds(0, others)], s_a.at[c % 4, p], r_a.at[c, p], exp_to[0])

    def pair_copy(c, slot):
        return rc(snd.at[slot, 0, me], g.at[c, y * 2 + zl, me], s_z.at[c], r_z.at[c], z_to)

    def pair_came(c):
        block = g.at[c, y * 2 + 1 - zl, me]
        return rc(block, block, s_z.at[c], r_z.at[c], z_to)

    def early_a(c):
        snd[c, 0] = contract(pls[0], tok[:, cols(c)], 1, 0).astype(BF).reshape(experts, BLOCK, width)
        g[c, y * 2 + zl, me] = snd[c, 0, me]
        for copy in a_copies(c, 0):
            copy.start()
        for dev in cross_to:
            rc(snd.at[c, 0, dev["exp"]], g.at[c, y * 2 + zl, me], s_a.at[c, 1], r_a.at[c, 1], dev).start()
        pair_copy(c, c).start()

    def stage_a(c, p):
        if p == 1:
            send_tokens(c).wait_recv()

            @pl.when(c == EARLY)
            def _():
                send_pl.wait_recv()

        source = (tok, tp)[p][:, cols(c)]
        made = contract(pls[p], source, 1, 0).astype(BF).reshape(experts, BLOCK, width)
        snd[c % 4, p] = made
        g[c, y * 2 + planes[p], me] = snd[c % 4, p, me]
        for copy in a_copies(c, p):
            copy.start()

    def early_only(c, do):
        if isinstance(c, int):
            do()
        else:
            pl.when(c < EARLY)(do)

    def b_copies(c):
        return [
            rc(g.at[c, y * 2 + p], g.at[c, y * 2 + p], s_b.at[c % 2, d, p], r_b.at[c, d, p], y_to[d])
            for d, p in ((0, 0), (1, 1), (0, 1), (1, 0))
        ]

    def b_arrived(c, d, p):
        at = (y_at(-1), y_at(1))[d] * 2 + p
        return rc(g.at[c, at], g.at[c, at], s_b.at[c % 2, d, p], r_b.at[c, d, p], y_to[d])

    def f_copies(c):
        out = []
        for d in range(2):
            at = (y_at(-1), y_at(1))[d] * 2 + d
            out.append(rc(g.at[c, at], g.at[c, at], s_f.at[c % 2, d], r_f.at[c, d], y_to[d]))
        return out

    def stage_b(c):
        for p in range(2):
            a_all(c, p).wait_recv()
        early_only(c, lambda: pair_came(c).wait_recv())
        for copy in b_copies(c):
            copy.start()

    def stage_f(c):
        copies = f_copies(c)
        for d in range(2):
            b_arrived(c, d, d).wait_recv()
            copies[d].start()

    def stage_w(c):
        b_arrived(c, 0, 1).wait_recv()
        b_arrived(c, 1, 0).wait_recv()
        for copy in f_copies(c):
            copy.wait_recv()
        grad = contract(g[c].reshape(2 * ys * slab, width), cp[...].reshape(2 * ys * slab, -1), 0, 0)
        acc[c % 4] = grad.reshape(2, 2, 2, width // 8, -1)
        for v in range(2):
            sb[c % 4, v] = acc[c % 4, v, 1 - r_bit[v]].astype(BF)
        for copy in d0_copies(c):
            copy.start()

    def d0_copies(c):
        return [rc(sb.at[c % 4, v], rb.at[c, v], s_d.at[c % 2, 0, v], r_d.at[c, 0, v], r_by[v]) for v in range(2)]

    def d1_copies(c):
        return [
            rc(rb.at[c, v, 1 - r_bit[1 - v]], rc1.at[c, v], s_d.at[c % 2, 1, v], r_d.at[c, 1, v], r_by[1 - v])
            for v in range(2)
        ]

    def stage_d(c):
        came, send = d0_copies(c), d1_copies(c)
        for v in range(2):
            came[v].wait_recv()
            q = 1 - r_bit[1 - v]
            rb[c, v, q] = (rb[c, v, q].astype(F32) + acc[c % 4, v, r_bit[v], q]).astype(BF)
            send[v].start()

    def g0_copies(c):
        out = []
        for v in range(2):
            piece = wg_out.at[c, v, r_bit[v], r_bit[1 - v]]
            out.append(rc(piece, piece, s_g.at[c % 2, 0, v], r_g.at[c, 0, v], r_by[1 - v]))
        return out

    def g1_copies(c):
        out = []
        for v in range(2):
            half = wg_out.at[c, v, r_bit[v]]
            out.append(rc(half, half, s_g.at[c % 2, 1, v], r_g.at[c, 1, v], r_by[v]))
        return out

    def stage_e(c):
        came, send = d1_copies(c), g0_copies(c)
        for v in range(2):
            came[v].wait_recv()
            h, q = r_bit[v], r_bit[1 - v]
            total = acc[c % 4, v, h, q] + rb[c, v, q].astype(F32) + rc1[c, v].astype(F32)
            wg_out[c, v, h, q] = total.astype(BF)
            send[v].start()

    def stage_g(c):
        came, send = g0_copies(c), g1_copies(c)
        for v in range(2):
            came[v].wait_recv()
            send[v].start()

    def stage_end(c):
        for copy in g1_copies(c):
            copy.wait_recv()

    def r0_copies(c):
        return [
            rc(prod.at[c % KEEP, (y_pair[v], y_far)[i] * 2 + v], rr.at[c, v, i], s_r.at[c % 2, i, v], r_r.at[c, i, v], y_by[v])
            for i in (1, 0)
            for v in range(2)
        ]

    def r1_copies(c):
        return [rc(rr.at[c, v, 1], rr1.at[c, v], s_r.at[c % 2, 2, v], r_r.at[c, 2, v], y_by[1 - v]) for v in range(2)]

    def stage_p(c):
        odd = lax.rem(c, 2)
        pair = c - odd
        weights = wv[pl.ds(pl.multiple_of(pair * width, 256), 2 * width), :]

        @pl.loop(0, ys)
        def _(i):
            s = odd * ys + i
            made = contract(cp[s].reshape(slab, -1), weights, 1, 1).astype(BF)
            for j in range(2):
                prod[lax.rem(pair + j, KEEP), s] = made[:, j * width : (j + 1) * width]

    def stage_r0(c):
        for copy in r0_copies(c):
            copy.start()

    def stage_r1(c):
        came, send = r0_copies(c), r1_copies(c)
        for v in range(2):
            came[v].wait_recv()
            mine = prod[c % KEEP, y_pair[1 - v] * 2 + v].astype(F32)
            rr[c, v, 1] = (rr[c, v, 1].astype(F32) + mine).astype(BF)
            send[v].start()

    def m_copies(c, d):
        return [rc(u.at[c % 4, d, dev["exp"]], x2.at[c, d, me], s_m.at[c % 2, d], r_m.at[c, d], dev) for dev in exp_to]

    def m_all(c, d):
        return rc(x2.at[c, d, pl.ds(0, others)], x2.at[c, d, pl.ds(0, others)], s_m.at[c % 2, d], r_m.at[c, d], exp_to[0])

    def stage_m(c):
        first_half, second = r0_copies(c), r1_copies(c)
        for d in range(2):
            first_half[2 + d].wait_recv()
            second[d].wait_recv()
            total = rr[c, d, 0].astype(F32) + prod[c % KEEP, y * 2 + d].astype(F32) + rr1[c, d].astype(F32)
            u[c % 4, d] = total.astype(BF).reshape(experts, BLOCK, width)
            x2[c, d, me] = u[c % 4, d, me]
            for copy in m_copies(c, d):
                copy.start()

    def n_copy(c):
        return rc(zs.at[c], zr.at[c], s_n.at[c % 2], r_n.at[c], z_to)

    def stage_n(c):
        for d in range(2):
            m_all(c, d).wait_recv()
        theirs = contract(pls[1], x2[c, planes[1]].reshape(slots, width), 0, 0)
        zs[c] = theirs.astype(BF)
        n_copy(c).start()
        zo[c] = contract(pls[0], x2[c, planes[0]].reshape(slots, width), 0, 0)

    def stage_o(c):
        n_copy(c).wait_recv()
        tg_out[:, cols(c)] = (zo[c] + zr[c].astype(F32)).astype(BF)

    def at(t, offset, stage):
        c = t - offset

        @pl.when((c >= 0) & (c < CHUNKS))
        def _():
            stage(c)

    def wait_sends(make):
        def stage(c):
            for copy in make(c):
                copy.wait_send()

        return stage

    def prepare():
        loads[2].wait()
        row = lax.broadcasted_iota(jnp.int32, (2 * ys * BLOCK, 2 * ys * slot_cap), 0)
        col = lax.broadcasted_iota(jnp.int32, (2 * ys * BLOCK, 2 * ys * slot_cap), 1)
        inner = lax.rem(row, BLOCK)
        spaced = jnp.where((col == (row // BLOCK) * slot_cap + inner) & (inner < slot_cap), 1.0, 0.0).astype(BF)

        @pl.loop(0, experts)
        def _(e):
            moved = contract(spaced, cn[e], 1, 0).astype(BF)
            for z in range(2):
                for yy in range(ys):
                    at = (z * ys + yy) * BLOCK
                    cp[yy * 2 + z, e] = moved[at : at + BLOCK]

    first = 3
    ticks = CHUNKS + max(first + 5, 7)

    early_a(0)
    send_pl.start()
    for c in range(1, EARLY):
        early_a(c)

    @pl.loop(EARLY, CHUNKS)
    def _(c):
        send_tokens(c).start()

    prepare()
    loads[3].wait()
    stage_b(0)
    a_all(0, 0).wait_send()
    a_all(0, 1).wait_send()
    pair_copy(0, 0).wait_send()

    @pl.loop(1, ticks)
    def _(t):
        at(t, first + 2, stage_m)
        at(t, 5, stage_g)
        at(t, first + 1, stage_r1)
        at(t, 4, stage_e)
        at(t, 1, stage_f)
        at(t, 3, stage_d)
        at(t, first, stage_r0)
        at(t, 0, stage_b)
        at(t, first + 3, stage_n)
        at(t, 2, stage_w)
        at(t, first + 4, stage_o)
        at(t, 6, stage_end)
        at(t, -2, functools.partial(stage_a, p=0))
        at(t, -2, functools.partial(stage_a, p=1))
        at(t, 0, wait_sends(lambda c: [a_all(c, 0), a_all(c, 1)]))
        at(t, 0, lambda c: early_only(c, lambda: pair_copy(c, c % 4).wait_send()))
        at(t, 1, wait_sends(lambda c: b_copies(c)))
        at(t, 2, wait_sends(lambda c: f_copies(c)))
        at(t, 3, wait_sends(lambda c: d0_copies(c)))
        at(t, 4, wait_sends(lambda c: d1_copies(c)))
        at(t, 5, wait_sends(lambda c: g0_copies(c)))
        at(t, 6, wait_sends(lambda c: g1_copies(c)))
        at(t, first + 1, wait_sends(lambda c: r0_copies(c)))
        at(t, first + 2, wait_sends(lambda c: r1_copies(c)))
        at(t, first + 3, wait_sends(lambda c: [m_all(c, 0), m_all(c, 1)]))
        at(t, first + 4, wait_sends(lambda c: [n_copy(c)]))
        at(t, first + 4, lambda c: pl.when(c >= EARLY)(lambda: send_tokens(c).wait_send()))
        at(t, first - 2, stage_p)

    send_pl.wait_send()


def solution(mesh):
    reps, experts, shards = (mesh.shape[a] for a in ("rep", "exp", "shard"))
    ys = shards // 2

    def body(tokens, routes, gate_weight, gate_cotangent):
        rows, features = tokens.shape
        hidden = gate_weight.shape[2]
        slot_cap = gate_cotangent.shape[1] // (experts * shards)
        width = features // CHUNKS
        n = CHUNKS
        slots = experts * BLOCK
        cotangent = gate_cotangent.reshape(experts, shards * slot_cap, hidden)
        vmem = lambda *shape: pltpu.VMEM(shape, BF)
        wide = lambda *shape: pltpu.VMEM(shape, F32)
        dma = lambda *shape: pltpu.SemaphoreType.DMA(shape)
        whole = pl.BlockSpec(memory_space=pltpu.VMEM)
        far = pl.BlockSpec(memory_space=pltpu.HBM)
        piece = width // 8
        scratch = [
            vmem(rows, features),
            pltpu.VMEM((2, rows), jnp.int32),
            vmem(experts, shards * slot_cap, hidden),
            vmem(shards, experts, BLOCK, hidden),
            vmem(features, hidden),
            vmem(2, slots, rows),
            vmem(rows, features),
            vmem(4, 2, experts, BLOCK, width),
            vmem(n, shards, experts, BLOCK, width),
            vmem(KEEP, shards, slots, width),
            vmem(n, 2, 2, slots, width),
            vmem(n, 2, slots, width),
            vmem(4, 2, experts, BLOCK, width),
            vmem(n, 2, experts, BLOCK, width),
            vmem(n, rows, width),
            wide(n, rows, width),
            vmem(n, rows, width),
            wide(4, 2, 2, 2, piece, hidden),
            vmem(4, 2, 2, piece, hidden),
            vmem(n, 2, 2, piece, hidden),
            vmem(n, 2, piece, hidden),
            dma(4), dma(2), dma(n), dma(n), dma(EARLY), dma(EARLY),
            dma(4, 2), dma(n, 2),
            dma(2, 2, 2), dma(n, 2, 2),
            dma(2, 2), dma(n, 2),
            dma(2, 3, 2), dma(n, 3, 2),
            dma(2, 2), dma(n, 2),
            dma(2), dma(n),
            dma(2, 2, 2), dma(n, 2, 2),
            dma(2, 2, 2), dma(n, 2, 2),
        ]
        token_grad, weight_grad = pl.pallas_call(
            functools.partial(kernel, (reps, experts, ys, slot_cap, width)),
            out_shape=(
                jax.ShapeDtypeStruct((rows, features), BF),
                jax.ShapeDtypeStruct((n, 2, 2, 2, piece, hidden), BF),
            ),
            in_specs=[far, far, far, far],
            out_specs=(whole, whole),
            scratch_shapes=scratch,
            compiler_params=pltpu.CompilerParams(
                collective_id=0, has_side_effects=True, vmem_limit_bytes=VMEM
            ),
            name="moe_gate_backward",
        )(*(pltpu.with_memory_space_constraint(a, pltpu.HBM) for a in (tokens, routes.T, cotangent, gate_weight[0])))
        return token_grad, weight_grad.reshape(1, features, hidden)

    spec = P(("rep", "exp", "shard"), None)
    return jax.shard_map(
        body,
        mesh=mesh,
        in_specs=(spec, spec, P("exp", None, "shard"), P("exp", "rep", "shard")),
        out_specs=(spec, P("exp", None, "shard")),
        check_vma=False,
    )
```

```python
import functools

import jax
import jax.numpy as jnp
from jax import lax
from jax.experimental import pallas as pl
from jax.experimental.pallas import tpu as pltpu
from jax.sharding import PartitionSpec as P

MESH = pl.DeviceIdType.MESH
BF = jnp.bfloat16
F32 = jnp.float32
CHUNKS = 16
EARLY = 3
KEEP = 8
VMEM = 50_000_000
BLOCK = 32


def contract(a, b, da, db):
    return lax.dot_general(a, b, (((da,), (db,)), ((), ())), preferred_element_type=F32)


def kernel(
    sizes, tok_hbm, routes_hbm, c_hbm, w_hbm, tg_out, wg_out,
    tok, routes, cn, cp, wv, pls, tp, snd, g, prod, rr, rr1, u, x2, zs, zo, zr, acc, sb, rb, rc1,
    load_sem, pl_sem, t_sem, t_rsem, s_z, r_z, s_a, r_a, s_b, r_b, s_f, r_f, s_r, r_r, s_m, r_m, s_n, r_n, s_d, r_d, s_g, r_g,
):
    reps, experts, ys, slot_cap, width = sizes
    rep, me, shard = lax.axis_index("rep"), lax.axis_index("exp"), lax.axis_index("shard")
    zl, y = shard // ys, lax.rem(shard, ys)
    y_at = lambda k: lax.rem(y + k + 4 * ys, ys)
    swap = lambda i: (i + 1 - 2 * lax.rem(i, 2), 3 - i)
    bits = lambda i: (lax.rem((i + 1) // 2, 2), i // 2)
    y_pair, r_pair = swap(y), swap(rep)
    y_far = lax.rem(y + 2, ys)
    r_bit = bits(rep)
    y_to = ({"shard": zl * ys + y_at(1)}, {"shard": zl * ys + y_at(-1)})
    y_by = tuple({"shard": zl * ys + i} for i in y_pair)
    r_by = tuple({"rep": i} for i in r_pair)
    z_to = {"shard": (1 - zl) * ys + y}
    exp_to = [{"exp": lax.rem(me + d, experts)} for d in range(1, experts)]
    others = experts - 1
    planes = (zl, 1 - zl)

    def rc(src, dst, ssem, rsem, dev):
        return pltpu.make_async_remote_copy(
            src_ref=src, dst_ref=dst, send_sem=ssem, recv_sem=rsem, device_id=dev, device_id_type=MESH
        )

    loads = [
        pltpu.make_async_copy(src, dst, load_sem.at[i])
        for i, (src, dst) in enumerate(((routes_hbm, routes), (tok_hbm, tok), (c_hbm, cn), (w_hbm, wv)))
    ]
    for load in loads:
        load.start()

    barrier = pltpu.get_barrier_semaphore()
    cross_to = [{**dev, **z_to} for dev in exp_to]
    peers = [*y_to, *r_by, z_to, *exp_to, *cross_to]
    for dev in peers:
        pl.semaphore_signal(barrier, inc=1, device_id=dev, device_id_type=MESH)

    loads[0].wait()
    rows = tok.shape[0]
    slots = experts * BLOCK
    name = lax.broadcasted_iota(jnp.int32, (experts, rows), 0)
    named = ((routes[0:1, :] == name) | (routes[1:2, :] == name)).astype(F32).astype(BF)
    before = (
        lax.broadcasted_iota(jnp.int32, (rows, rows), 0) < lax.broadcasted_iota(jnp.int32, (rows, rows), 1)
    ).astype(F32).astype(BF)
    position = contract(named, before, 1, 0).astype(BF)
    spread = (
        lax.broadcasted_iota(jnp.int32, (slots, experts), 0) // BLOCK
        == lax.broadcasted_iota(jnp.int32, (slots, experts), 1)
    ).astype(F32).astype(BF)
    slot_of = lax.rem(lax.broadcasted_iota(jnp.int32, (slots, rows), 0), BLOCK).astype(F32)
    hit = contract(spread, named, 1, 0)
    where = contract(spread, position, 1, 0)
    pls[0] = jnp.where(where == slot_of, hit, 0.0).astype(BF)

    pl.semaphore_wait(barrier, len(peers))

    send_pl = rc(pls.at[0], pls.at[1], pl_sem.at[0], pl_sem.at[1], z_to)
    loads[1].wait()
    cols = lambda c: pl.ds(pl.multiple_of(c * width, 128), width)

    def send_tokens(c):
        return rc(tok.at[:, cols(c)], tp.at[:, cols(c)], t_sem.at[c], t_rsem.at[c], z_to)

    slab = slots

    def a_copies(c, p):
        at = y * 2 + planes[p]
        return [
            rc(snd.at[c % 4, p, dev["exp"]], g.at[c, at, me], s_a.at[c % 4, p], r_a.at[c, p], dev) for dev in exp_to
        ]

    def a_all(c, p):
        at = y * 2 + planes[p]
        return rc(g.at[c, at, pl.ds(0, others)], g.at[c, at, pl.ds(0, others)], s_a.at[c % 4, p], r_a.at[c, p], exp_to[0])

    def pair_copy(c, slot):
        return rc(snd.at[slot, 0, me], g.at[c, y * 2 + zl, me], s_z.at[c], r_z.at[c], z_to)

    def pair_came(c):
        block = g.at[c, y * 2 + 1 - zl, me]
        return rc(block, block, s_z.at[c], r_z.at[c], z_to)

    def early_a(c):
        snd[c, 0] = contract(pls[0], tok[:, cols(c)], 1, 0).astype(BF).reshape(experts, BLOCK, width)
        g[c, y * 2 + zl, me] = snd[c, 0, me]
        for copy in a_copies(c, 0):
            copy.start()
        for dev in cross_to:
            rc(snd.at[c, 0, dev["exp"]], g.at[c, y * 2 + zl, me], s_a.at[c, 1], r_a.at[c, 1], dev).start()
        pair_copy(c, c).start()

    def stage_a(c, p):
        if p == 1:
            send_tokens(c).wait_recv()

            @pl.when(c == EARLY)
            def _():
                send_pl.wait_recv()

        source = (tok, tp)[p][:, cols(c)]
        made = contract(pls[p], source, 1, 0).astype(BF).reshape(experts, BLOCK, width)
        snd[c % 4, p] = made
        g[c, y * 2 + planes[p], me] = snd[c % 4, p, me]
        for copy in a_copies(c, p):
            copy.start()

    def early_only(c, do):
        if isinstance(c, int):
            do()
        else:
            pl.when(c < EARLY)(do)

    def b_copies(c):
        return [
            rc(g.at[c, y * 2 + p], g.at[c, y * 2 + p], s_b.at[c % 2, d, p], r_b.at[c, d, p], y_to[d])
            for d, p in ((0, 0), (1, 1), (0, 1), (1, 0))
        ]

    def b_arrived(c, d, p):
        at = (y_at(-1), y_at(1))[d] * 2 + p
        return rc(g.at[c, at], g.at[c, at], s_b.at[c % 2, d, p], r_b.at[c, d, p], y_to[d])

    def f_copies(c):
        out = []
        for d in range(2):
            at = (y_at(-1), y_at(1))[d] * 2 + d
            out.append(rc(g.at[c, at], g.at[c, at], s_f.at[c % 2, d], r_f.at[c, d], y_to[d]))
        return out

    def stage_b(c):
        for p in range(2):
            a_all(c, p).wait_recv()
        early_only(c, lambda: pair_came(c).wait_recv())
        for copy in b_copies(c):
            copy.start()

    def stage_f(c):
        copies = f_copies(c)
        for d in range(2):
            b_arrived(c, d, d).wait_recv()
            copies[d].start()

    def stage_w(c):
        b_arrived(c, 0, 1).wait_recv()
        b_arrived(c, 1, 0).wait_recv()
        for copy in f_copies(c):
            copy.wait_recv()
        grad = contract(g[c].reshape(2 * ys * slab, width), cp[...].reshape(2 * ys * slab, -1), 0, 0)
        acc[c % 4] = grad.reshape(2, 2, 2, width // 8, -1)
        for v in range(2):
            sb[c % 4, v] = acc[c % 4, v, 1 - r_bit[v]].astype(BF)
        for copy in d0_copies(c):
            copy.start()

    def d0_copies(c):
        out = []
        for i in range(2):
            for v in range(2):
                q = (1 - r_bit[1 - v], r_bit[1 - v])[i]
                out.append(rc(sb.at[c % 4, v, q], rb.at[c, v, q], s_d.at[c % 2, 2 * i, v], r_d.at[c, 2 * i, v], r_by[v]))
        return out

    def d1_copies(c):
        return [
            rc(rb.at[c, v, 1 - r_bit[1 - v]], rc1.at[c, v], s_d.at[c % 2, 1, v], r_d.at[c, 1, v], r_by[1 - v])
            for v in range(2)
        ]

    def stage_d(c):
        came, send = d0_copies(c), d1_copies(c)
        for v in range(2):
            came[v].wait_recv()
            q = 1 - r_bit[1 - v]
            rb[c, v, q] = (rb[c, v, q].astype(F32) + acc[c % 4, v, r_bit[v], q]).astype(BF)
            send[v].start()

    def g0_copies(c):
        out = []
        for v in range(2):
            piece = wg_out.at[c, v, r_bit[v], r_bit[1 - v]]
            out.append(rc(piece, piece, s_g.at[c % 2, 0, v], r_g.at[c, 0, v], r_by[1 - v]))
        return out

    def own_copies(c):
        out = []
        for v in range(2):
            piece = wg_out.at[c, v, r_bit[v], r_bit[1 - v]]
            out.append(rc(piece, piece, s_g.at[c % 2, 2, v], r_g.at[c, 2, v], r_by[v]))
        return out

    def g1_copies(c):
        out = []
        for v in range(2):
            piece = wg_out.at[c, v, r_bit[v], 1 - r_bit[1 - v]]
            out.append(rc(piece, piece, s_g.at[c % 2, 1, v], r_g.at[c, 1, v], r_by[v]))
        return out

    def stage_e(c):
        came, rest, send, own = d1_copies(c), d0_copies(c), g0_copies(c), own_copies(c)
        for v in range(2):
            rest[2 + v].wait_recv()
            came[v].wait_recv()
            h, q = r_bit[v], r_bit[1 - v]
            total = acc[c % 4, v, h, q] + rb[c, v, q].astype(F32) + rc1[c, v].astype(F32)
            wg_out[c, v, h, q] = total.astype(BF)
            send[v].start()
        for copy in own:
            copy.start()

    def stage_g(c):
        came, send = g0_copies(c), g1_copies(c)
        for v in range(2):
            came[v].wait_recv()
            send[v].start()

    def stage_end(c):
        for copy in own_copies(c) + g1_copies(c):
            copy.wait_recv()

    def r0_copies(c):
        return [
            rc(prod.at[c % KEEP, (y_pair[v], y_far)[i] * 2 + v], rr.at[c, v, i], s_r.at[c % 2, i, v], r_r.at[c, i, v], y_by[v])
            for i in (1, 0)
            for v in range(2)
        ]

    def r1_copies(c):
        return [rc(rr.at[c, v, 1], rr1.at[c, v], s_r.at[c % 2, 2, v], r_r.at[c, 2, v], y_by[1 - v]) for v in range(2)]

    def stage_p(c):
        odd = lax.rem(c, 2)
        pair = c - odd
        weights = wv[pl.ds(pl.multiple_of(pair * width, 256), 2 * width), :]

        @pl.loop(0, ys)
        def _(i):
            s = odd * ys + i
            made = contract(cp[s].reshape(slab, -1), weights, 1, 1).astype(BF)
            for j in range(2):
                prod[lax.rem(pair + j, KEEP), s] = made[:, j * width : (j + 1) * width]

    def stage_r0(c):
        for copy in r0_copies(c):
            copy.start()

    def stage_r1(c):
        came, send = r0_copies(c), r1_copies(c)
        for v in range(2):
            came[v].wait_recv()
            mine = prod[c % KEEP, y_pair[1 - v] * 2 + v].astype(F32)
            rr[c, v, 1] = (rr[c, v, 1].astype(F32) + mine).astype(BF)
            send[v].start()

    def m_copies(c, d):
        return [rc(u.at[c % 4, d, dev["exp"]], x2.at[c, d, me], s_m.at[c % 2, d], r_m.at[c, d], dev) for dev in exp_to]

    def m_all(c, d):
        return rc(x2.at[c, d, pl.ds(0, others)], x2.at[c, d, pl.ds(0, others)], s_m.at[c % 2, d], r_m.at[c, d], exp_to[0])

    def stage_m(c):
        first_half, second = r0_copies(c), r1_copies(c)
        for d in range(2):
            first_half[2 + d].wait_recv()
            second[d].wait_recv()
            total = rr[c, d, 0].astype(F32) + prod[c % KEEP, y * 2 + d].astype(F32) + rr1[c, d].astype(F32)
            u[c % 4, d] = total.astype(BF).reshape(experts, BLOCK, width)
            x2[c, d, me] = u[c % 4, d, me]
            for copy in m_copies(c, d):
                copy.start()

    def n_copy(c):
        return rc(zs.at[c], zr.at[c], s_n.at[c % 2], r_n.at[c], z_to)

    def stage_n(c):
        for d in range(2):
            m_all(c, d).wait_recv()
        theirs = contract(pls[1], x2[c, planes[1]].reshape(slots, width), 0, 0)
        zs[c] = theirs.astype(BF)
        n_copy(c).start()
        zo[c] = contract(pls[0], x2[c, planes[0]].reshape(slots, width), 0, 0)

    def stage_o(c):
        n_copy(c).wait_recv()
        tg_out[:, cols(c)] = (zo[c] + zr[c].astype(F32)).astype(BF)

    def at(t, offset, stage):
        c = t - offset

        @pl.when((c >= 0) & (c < CHUNKS))
        def _():
            stage(c)

    def wait_sends(make):
        def stage(c):
            for copy in make(c):
                copy.wait_send()

        return stage

    def prepare():
        loads[2].wait()
        row = lax.broadcasted_iota(jnp.int32, (2 * ys * BLOCK, 2 * ys * slot_cap), 0)
        col = lax.broadcasted_iota(jnp.int32, (2 * ys * BLOCK, 2 * ys * slot_cap), 1)
        inner = lax.rem(row, BLOCK)
        spaced = jnp.where((col == (row // BLOCK) * slot_cap + inner) & (inner < slot_cap), 1.0, 0.0).astype(BF)

        @pl.loop(0, experts)
        def _(e):
            moved = contract(spaced, cn[e], 1, 0).astype(BF)
            for z in range(2):
                for yy in range(ys):
                    at = (z * ys + yy) * BLOCK
                    cp[yy * 2 + z, e] = moved[at : at + BLOCK]

    first = 3
    ticks = CHUNKS + max(first + 5, 7)

    early_a(0)
    send_pl.start()
    for c in range(1, EARLY):
        early_a(c)

    @pl.loop(EARLY, CHUNKS)
    def _(c):
        send_tokens(c).start()

    prepare()
    loads[3].wait()
    stage_b(0)
    a_all(0, 0).wait_send()
    a_all(0, 1).wait_send()
    pair_copy(0, 0).wait_send()

    @pl.loop(1, ticks)
    def _(t):
        at(t, first + 2, stage_m)
        at(t, 5, stage_g)
        at(t, first + 1, stage_r1)
        at(t, 4, stage_e)
        at(t, 1, stage_f)
        at(t, 3, stage_d)
        at(t, first, stage_r0)
        at(t, 0, stage_b)
        at(t, first + 3, stage_n)
        at(t, 2, stage_w)
        at(t, first + 4, stage_o)
        at(t, 6, stage_end)
        at(t, -2, functools.partial(stage_a, p=0))
        at(t, -2, functools.partial(stage_a, p=1))
        at(t, 0, wait_sends(lambda c: [a_all(c, 0), a_all(c, 1)]))
        at(t, 0, lambda c: early_only(c, lambda: pair_copy(c, c % 4).wait_send()))
        at(t, 1, wait_sends(lambda c: b_copies(c)))
        at(t, 2, wait_sends(lambda c: f_copies(c)))
        at(t, 3, wait_sends(lambda c: d0_copies(c)))
        at(t, 4, wait_sends(lambda c: d1_copies(c)))
        at(t, 5, wait_sends(lambda c: g0_copies(c) + own_copies(c)))
        at(t, 6, wait_sends(lambda c: g1_copies(c)))
        at(t, first + 1, wait_sends(lambda c: r0_copies(c)))
        at(t, first + 2, wait_sends(lambda c: r1_copies(c)))
        at(t, first + 3, wait_sends(lambda c: [m_all(c, 0), m_all(c, 1)]))
        at(t, first + 4, wait_sends(lambda c: [n_copy(c)]))
        at(t, first + 4, lambda c: pl.when(c >= EARLY)(lambda: send_tokens(c).wait_send()))
        at(t, first - 2, stage_p)

    send_pl.wait_send()


def solution(mesh):
    reps, experts, shards = (mesh.shape[a] for a in ("rep", "exp", "shard"))
    ys = shards // 2

    def body(tokens, routes, gate_weight, gate_cotangent):
        rows, features = tokens.shape
        hidden = gate_weight.shape[2]
        slot_cap = gate_cotangent.shape[1] // (experts * shards)
        width = features // CHUNKS
        n = CHUNKS
        slots = experts * BLOCK
        cotangent = gate_cotangent.reshape(experts, shards * slot_cap, hidden)
        vmem = lambda *shape: pltpu.VMEM(shape, BF)
        wide = lambda *shape: pltpu.VMEM(shape, F32)
        dma = lambda *shape: pltpu.SemaphoreType.DMA(shape)
        whole = pl.BlockSpec(memory_space=pltpu.VMEM)
        far = pl.BlockSpec(memory_space=pltpu.HBM)
        piece = width // 8
        scratch = [
            vmem(rows, features),
            pltpu.VMEM((2, rows), jnp.int32),
            vmem(experts, shards * slot_cap, hidden),
            vmem(shards, experts, BLOCK, hidden),
            vmem(features, hidden),
            vmem(2, slots, rows),
            vmem(rows, features),
            vmem(4, 2, experts, BLOCK, width),
            vmem(n, shards, experts, BLOCK, width),
            vmem(KEEP, shards, slots, width),
            vmem(n, 2, 2, slots, width),
            vmem(n, 2, slots, width),
            vmem(4, 2, experts, BLOCK, width),
            vmem(n, 2, experts, BLOCK, width),
            vmem(n, rows, width),
            wide(n, rows, width),
            vmem(n, rows, width),
            wide(4, 2, 2, 2, piece, hidden),
            vmem(4, 2, 2, piece, hidden),
            vmem(n, 2, 2, piece, hidden),
            vmem(n, 2, piece, hidden),
            dma(4), dma(2), dma(n), dma(n), dma(EARLY), dma(EARLY),
            dma(4, 2), dma(n, 2),
            dma(2, 2, 2), dma(n, 2, 2),
            dma(2, 2), dma(n, 2),
            dma(2, 3, 2), dma(n, 3, 2),
            dma(2, 2), dma(n, 2),
            dma(2), dma(n),
            dma(2, 3, 2), dma(n, 3, 2),
            dma(2, 3, 2), dma(n, 3, 2),
        ]
        token_grad, weight_grad = pl.pallas_call(
            functools.partial(kernel, (reps, experts, ys, slot_cap, width)),
            out_shape=(
                jax.ShapeDtypeStruct((rows, features), BF),
                jax.ShapeDtypeStruct((n, 2, 2, 2, piece, hidden), BF),
            ),
            in_specs=[far, far, far, far],
            out_specs=(whole, whole),
            scratch_shapes=scratch,
            compiler_params=pltpu.CompilerParams(
                collective_id=0, has_side_effects=True, vmem_limit_bytes=VMEM
            ),
            name="moe_gate_backward",
        )(*(pltpu.with_memory_space_constraint(a, pltpu.HBM) for a in (tokens, routes.T, cotangent, gate_weight[0])))
        return token_grad, weight_grad.reshape(1, features, hidden)

    spec = P(("rep", "exp", "shard"), None)
    return jax.shard_map(
        body,
        mesh=mesh,
        in_specs=(spec, spec, P("exp", None, "shard"), P("exp", "rep", "shard")),
        out_specs=(spec, P("exp", None, "shard")),
        check_vma=False,
    )
```
